512 devices in a mesh: dp: 16 (over y, x), tensor: 32 (over z, core).
Axes of the slice: x: 4, y: 4, z: 16, core: 2. Of those that a mesh axis runs over, the one named last changes fastest.
Arguments:
- logits: bfloat16 [4096, 152064], P('dp', 'tensor'), may hold values from -120 to 256
- child_ids: int32 [4096, 64], P('dp'), may hold values from 0 to 152063
- leaf_counts: int32 [4096, 64], P('dp'), may hold values from 1 to 1024
- leaf_valid: int32 [4096], P('dp'), may hold values from 1 to 64
- leaf_temp: float32 [4096], P('dp'), may hold values from 0.5 to 2
- leaf_owner: int32 [4096], P('dp'), may hold values from 0 to 4095, as said below
Outputs:
- gradient: bfloat16 [4096, 152064], P('dp', 'tensor')
- row_loss: float32 [4096], P('dp')
- mean_loss: float32 [], replicated
The draws below stay inside these ranges and needn't reach their ends.
Inputs may be any that keep to these rules, and one draw needn't show every extreme that they name: `leaf_owner`: every position is named by exactly one leaf row. Of the leaf rows of one dp index, exactly 16 name positions of each owner index.
All inputs are finite; a program needn't handle non-finite values.
Results may differ from the reference program's by a relative error of at most 0.001.
Values may be sent and summed in bfloat16 or wider, within the bound.
A program may use at most 64 MiB of HBM per device.

```python
import math
import jax
import jax.numpy as jnp
from jax import lax

VOCAB = 152064
CHILD = 64
POS_DEV = 256
POSITIONS = 4096
N_DP = 16


def draw_logits(key, part):
    subkeys = jax.random.split(jax.random.fold_in(key, 7), 3)
    row_index = jnp.arange(POSITIONS, dtype=jnp.float32)
    row_scale = jnp.exp(jax.random.uniform(subkeys[0], (POSITIONS,), minval=0.0, maxval=math.log(3.2))) * (1.0 + 2.0 * row_index / POSITIONS)
    column_scale = jnp.exp(jax.random.uniform(subkeys[1], (VOCAB,), minval=0.0, maxval=math.log(3.2)))
    base_draw = jnp.clip(jax.random.normal(subkeys[2], (POSITIONS, VOCAB)), -4.5, 4.5)
    values = 0.6 * base_draw * row_scale[:, None] * column_scale[None, :]
    return values.astype(jnp.bfloat16)


def draw_leaf_owner(key, part):
    subkeys = jax.random.split(jax.random.fold_in(key, 13), 3)
    block_rows = POS_DEV // N_DP
    shifts = jax.random.permutation(subkeys[0], N_DP).astype(jnp.int32)
    source_dev = jnp.arange(N_DP, dtype=jnp.int32)[:, None]
    slot_index = jnp.arange(POS_DEV, dtype=jnp.int32)[None, :]
    block_index = slot_index // block_rows
    owner_dev = (source_dev + shifts[block_index]) % N_DP
    orders = jax.vmap(lambda subkey: jax.random.permutation(subkey, POS_DEV))(jax.random.split(subkeys[1], N_DP)).astype(jnp.int32)
    local_slot = orders[owner_dev, jnp.broadcast_to(slot_index, (N_DP, POS_DEV))]
    owners = owner_dev * POS_DEV + local_slot
    mixing = jax.vmap(lambda subkey: jax.random.permutation(subkey, POS_DEV))(jax.random.split(subkeys[2], N_DP))
    owners = jnp.take_along_axis(owners, mixing, axis=1)
    return owners.reshape(-1).astype(jnp.int32)


def plant(result, rng, least, high):
    place = [jax.random.randint(jax.random.fold_in(rng, axis), (), 0, length) for axis, length in enumerate(result.shape)]
    main_axis = result.shape.index(max(result.shape))
    neighbour = place[:main_axis] + [(place[main_axis] + 1) % result.shape[main_axis]] + place[main_axis + 1:]
    return result.at[tuple(place)].set(least).at[tuple(neighbour)].set(high)


def level_of(own_key, extent, shards, smallest, high):
    def one(axis_at, blocks):
        draws = jax.random.uniform(jax.random.fold_in(jax.random.fold_in(own_key, 6), axis_at), (blocks,), jnp.float32, smallest / len(shards), high / len(shards))
        return jnp.repeat(jnp.exp(draws), extent[axis_at] // blocks).reshape((-1,) + (1,) * (len(extent) - axis_at - 1))

    gain = one(*shards[0])
    for cut in shards[1:]:
        gain = gain * one(*cut)
    return gain


def setup_inputs(seed: int = 0) -> dict:
    key_list = jax.random.split(jax.random.key(seed), 7)
    return {
        "logits": draw_logits(jax.random.fold_in(key_list[6], 71), 0),
        "child_ids": plant(jax.random.randint(key_list[1], (POSITIONS, CHILD), 0, VOCAB), jax.random.fold_in(key_list[1], 1), 0, VOCAB - 1).astype(jnp.int32),
        "leaf_counts": plant(jax.random.randint(key_list[2], (POSITIONS, CHILD), 1, 1025), jax.random.fold_in(key_list[2], 1), 1, 1024).astype(jnp.int32),
        "leaf_valid": plant(jax.random.randint(key_list[3], (POSITIONS,), 1, CHILD + 1), jax.random.fold_in(key_list[3], 1), 1, CHILD).astype(jnp.int32),
        "leaf_temp": jnp.clip(jnp.exp(math.log(2.0) - 1.3862944 * jax.random.uniform(key_list[4], (POSITIONS,), jnp.float32) ** level_of(key_list[4], (POSITIONS,), ((0, 16),), -0.2, 0.2)), 0.5, 2.0),
        "leaf_owner": draw_leaf_owner(jax.random.fold_in(key_list[6], 71), 0),
    }


def reference(logits, child_ids, leaf_counts, leaf_valid, leaf_temp, leaf_owner):
    slot_index = jnp.arange(CHILD, dtype=jnp.int32)
    in_use = slot_index[None, :] < leaf_valid[:, None]
    powered = jnp.exp(jnp.log(leaf_counts.astype(jnp.float32)) * leaf_temp[:, None])
    weights = jnp.where(in_use, powered, jnp.float32(0.0))
    placed = jnp.zeros((POSITIONS, CHILD), jnp.float32).at[leaf_owner].add(weights)
    targets = placed / jnp.sum(placed, axis=1)[:, None]

    def per_block(pieces):
        block_logits, block_targets, block_ids = pieces
        values = block_logits.astype(jnp.float32)
        row_top = jnp.max(values, axis=1)
        shifted = jnp.exp(values - row_top[:, None])
        sumexp = jnp.sum(shifted, axis=1)
        picked = jnp.sum(block_targets * jnp.take_along_axis(values, block_ids, axis=1), axis=1)
        losses = row_top + jnp.log(sumexp) - picked
        row_index = jnp.arange(block_ids.shape[0], dtype=jnp.int32)[:, None]
        target_dense = jnp.zeros_like(values).at[row_index, block_ids].add(block_targets)
        gradient = (shifted / sumexp[:, None] - target_dense).astype(jnp.bfloat16)
        return gradient, losses

    gradient, losses = lax.map(per_block, (logits.reshape(N_DP, POS_DEV, VOCAB), targets.reshape(N_DP, POS_DEV, CHILD), child_ids.reshape(N_DP, POS_DEV, CHILD)))
    row_loss = losses.reshape(POSITIONS)
    mean_loss = jnp.sum(row_loss) / POSITIONS
    return gradient.reshape(POSITIONS, VOCAB), row_loss, mean_loss
```

```python
import functools

import jax
import jax.numpy as jnp
from jax import lax
from jax.experimental import pallas as pl
from jax.experimental.pallas import tpu as pltpu
from jax.sharding import PartitionSpec as P

MESH = pl.DeviceIdType.MESH
F32 = jnp.float32
BF16 = jnp.bfloat16
LANES = 128
WIDE = 256
CHUNK = 176


def dot_nt(lhs, rhs):
    return lax.dot_general(lhs, rhs, (((1,), (1,)), ((), ())), preferred_element_type=F32)


def split(value):
    high = value.astype(BF16)
    rest = value - high.astype(F32)
    middle = rest.astype(BF16)
    return high, middle, (rest - middle.astype(F32)).astype(BF16)


def iota(shape, dim):
    return lax.broadcasted_iota(jnp.int32, shape, dim)


def kernel(
    groups, shards,
    x_hbm, ids_ref, count_ref, valid_ref, temp_ref, owner_ref,
    grad_hbm, loss_ref, mean_ref,
    xs, es, dense, spread, gout, outbuf, inbuf, placed, ids_rows,
    stat_send, stat_buf, pick_send, pick_buf, mean_send, mean_buf,
    x_sem, grad_sem, send_sem, route_sem, stat_sem, pick_sem, mean_sem,
):
    cols, pos = x_hbm.shape
    child = ids_ref.shape[0]
    cap = pos // groups
    my_dp = lax.axis_index("dp")
    my_t = lax.axis_index("tensor")
    heads = pl.cdiv(cols, WIDE)

    x_copy = pltpu.make_async_copy(x_hbm, xs, x_sem)
    x_copy.start()

    barrier = pltpu.get_barrier_semaphore()

    def greet_dp(k, _):
        pl.semaphore_signal(barrier, inc=1, device_id={"dp": lax.rem(my_dp + k, groups)}, device_id_type=MESH)
        return 0

    def greet_t(k, _):
        pl.semaphore_signal(barrier, inc=1, device_id={"tensor": lax.rem(my_t + k, shards)}, device_id_type=MESH)
        return 0

    lax.fori_loop(1, groups, greet_dp, 0)
    lax.fori_loop(1, shards, greet_t, 0)

    powered = jnp.exp(jnp.log(count_ref[...].astype(F32)) * temp_ref[...])
    weights = jnp.where(iota((child, pos), 0) < valid_ref[...], powered, 0.0)
    share = weights / jnp.sum(weights, axis=0, keepdims=True)
    owner = owner_ref[...]
    shift = pos.bit_length() - 1
    owner_dp = lax.shift_right_logical(owner, shift)
    place = lax.bitwise_and(owner, pos - 1)
    member = jnp.where(iota((groups, pos), 0) == owner_dp, 1.0, 0.0).astype(F32)
    before = jnp.where(iota((pos, pos), 0) < iota((pos, pos), 1), 1.0, 0.0).astype(BF16)
    earlier = jnp.dot(member.astype(BF16), before, preferred_element_type=F32)
    rank = jnp.sum(member * earlier, axis=0, keepdims=True)
    target_row = owner_dp * cap + rank.astype(jnp.int32)
    sender = jnp.where(iota((pos, pos), 0) == target_row, 1.0, 0.0).astype(BF16)
    high, middle, low = split(share)
    place_rows = jnp.broadcast_to(place.astype(F32), (child, pos)).astype(BF16)
    none = jnp.zeros_like(low)
    outgoing = dot_nt(sender, jnp.concatenate([high, place_rows], axis=0))
    outgoing = outgoing + dot_nt(sender, jnp.concatenate([middle, none], axis=0))
    outgoing = outgoing + dot_nt(sender, jnp.concatenate([low, none], axis=0))
    outbuf[...] = outgoing.reshape(groups, cap, 2 * child)

    local = ids_ref[...] - my_t * cols
    ids_rows[...] = jnp.transpose(jnp.concatenate([local, local], axis=0))

    x_copy.wait()
    steps = cols // CHUNK

    def part(g):
        return pl.ds(pl.multiple_of(g * CHUNK, CHUNK), CHUNK)

    def fold(value):
        return value.reshape(CHUNK // 8, 8, pos)

    def tops(g, top):
        return jnp.maximum(top, jnp.max(fold(xs[part(g), :].astype(F32)), axis=0))

    top = lax.fori_loop(1, steps, tops, jnp.max(fold(xs[0:CHUNK, :].astype(F32)), axis=0))
    top = jnp.max(top, axis=0, keepdims=True)

    def sums(g, total):
        powers = jnp.exp(xs[part(g), :].astype(F32) - top)
        es[part(g), :] = powers
        return total + jnp.sum(fold(powers), axis=0)

    total = lax.fori_loop(0, steps, sums, jnp.zeros((8, pos), F32))
    own_stats = jnp.concatenate([top, jnp.sum(total, axis=0, keepdims=True)], axis=0)
    stat_send[...] = own_stats
    stat_buf[pl.ds(my_t, 1)] = own_stats.reshape(1, 2, pos)

    pl.semaphore_wait(barrier, groups - 1 + shards - 1)

    def route(k, _):
        peer = lax.rem(my_dp + k, groups)
        pltpu.make_async_remote_copy(
            outbuf.at[peer], inbuf.at[my_dp], send_sem.at[0], route_sem,
            device_id={"dp": peer}, device_id_type=MESH,
        ).start()
        return 0

    def cast(source, buffer, slot, sem, axis, me, count):
        def one(k, _):
            pltpu.make_async_remote_copy(
                source, buffer.at[me], send_sem.at[slot], sem,
                device_id={axis: lax.rem(me + k, count)}, device_id_type=MESH,
            ).start()
            return 0

        lax.fori_loop(1, count, one, 0)

    def take(buffer, count, sem):
        piece = buffer.at[pl.ds(0, count)]
        pltpu.make_async_copy(piece, piece, sem).wait()

    lax.fori_loop(1, groups, route, 0)
    cast(stat_send, stat_buf, 1, stat_sem, "tensor", my_t, shards)
    inbuf[pl.ds(my_dp, 1)] = outbuf[pl.ds(my_dp, 1)]

    take(inbuf, groups - 1, route_sem)
    turned = jnp.transpose(inbuf[...].reshape(pos, 2 * child))
    high, middle, low = split(turned[:child])
    label = turned[child : child + 1].astype(jnp.int32)
    receiver = jnp.where(iota((pos, pos), 0) == label, 1.0, 0.0).astype(BF16)
    placed[...] = dot_nt(receiver, jnp.concatenate([high, middle, low, low], axis=0))

    block = 8
    width = block * child
    lane = iota((block, LANES), 1)
    half = (lane >= child).astype(jnp.int32)
    row8 = iota((block, LANES), 0)
    per = LANES // child
    pieces = width // LANES
    spread_rows = iota((WIDE, width), 0)

    def target_rows(g, _):
        rows = pl.ds(pl.multiple_of(g * block, block), block)
        local = ids_rows[rows, :]
        head = lax.shift_right_arithmetic(local, 8)
        rest = lax.bitwise_and(local, WIDE - 1)
        parts = placed[rows, 0:LANES]
        swapped = pltpu.roll(parts, child, 1)
        high2 = jnp.where(lane < child, parts, swapped)
        middle2 = jnp.where(lane < child, swapped, parts)
        low2 = placed[rows, LANES : 2 * LANES]
        heads_at, rests_at = [], []
        for c in range(pieces):
            own = row8 == per * c + half
            heads_at.append(jnp.where(own, head, -1))
            rests_at.append(jnp.sum(jnp.where(own, rest, 0), axis=0, keepdims=True))
        onehot = jnp.where(spread_rows == jnp.concatenate(rests_at, axis=1), 1.0, 0.0).astype(BF16)
        hits = [[at == h for at in heads_at] for h in range(heads)]
        found = jnp.zeros((heads * block, WIDE), F32)
        for value in (high2, middle2, low2):
            chosen = [jnp.concatenate([jnp.where(at, value, 0.0) for at in hit], axis=1) for hit in hits]
            found = found + dot_nt(jnp.concatenate(chosen, axis=0).astype(BF16), onehot)
        for h in range(heads):
            dense[rows, h * WIDE : (h + 1) * WIDE] = found[h * block : (h + 1) * block]
        return 0

    lax.fori_loop(0, pos // block, target_rows, 0)

    def turn(b, total):
        at = pl.multiple_of(b * LANES, LANES)
        tile = jnp.transpose(dense[:, pl.ds(at, LANES)])
        spread[pl.ds(at, LANES), :] = tile
        product = tile * xs[pl.ds(at, LANES), :].astype(F32)
        return total + jnp.sum(product.reshape(LANES // 8, 8, pos), axis=0)

    whole = cols // LANES
    total = lax.fori_loop(0, whole, turn, jnp.zeros((8, pos), F32))
    left = cols - whole * LANES
    if left:
        tile = jnp.transpose(dense[:, whole * LANES : (whole + 1) * LANES])[:left]
        spread[whole * LANES : cols, :] = tile
        product = tile * xs[whole * LANES : cols, :].astype(F32)
        total = total + jnp.sum(product.reshape(left // 8, 8, pos), axis=0)
    own_pick = jnp.sum(total, axis=0, keepdims=True)
    pick_send[...] = own_pick
    pick_buf[pl.ds(my_t, 1)] = own_pick.reshape(1, 1, pos)
    cast(pick_send, pick_buf, 2, pick_sem, "tensor", my_t, shards)

    take(stat_buf, shards - 1, stat_sem)
    every_top, every_sum = stat_buf[:, 0, :], stat_buf[:, 1, :]
    peak = jnp.max(every_top, axis=0, keepdims=True)
    whole_sum = jnp.sum(every_sum * jnp.exp(every_top - peak), axis=0, keepdims=True)
    scale = jnp.exp(top - peak) / whole_sum

    def gradient(g, _):
        gout[part(g), :] = (es[part(g), :] * scale - spread[part(g), :]).astype(gout.dtype)
        return 0

    lax.fori_loop(0, steps, gradient, 0)
    grad_copy = pltpu.make_async_copy(gout, grad_hbm, grad_sem)
    grad_copy.start()

    take(pick_buf, shards - 1, pick_sem)
    loss = peak + jnp.log(whole_sum) - jnp.sum(pick_buf[...], axis=0)
    loss_ref[...] = loss
    own_mean = jnp.broadcast_to(jnp.sum(loss, axis=1, keepdims=True), (1, LANES))
    mean_send[...] = own_mean
    mean_buf[pl.ds(my_dp, 1)] = own_mean.reshape(1, 1, LANES)
    cast(mean_send, mean_buf, 3, mean_sem, "dp", my_dp, groups)
    take(mean_buf, groups - 1, mean_sem)
    mean_ref[...] = jnp.sum(mean_buf[...], axis=0) / (groups * pos)

    take(outbuf, groups - 1, send_sem.at[0])
    take(stat_buf, shards - 1, send_sem.at[1])
    take(pick_buf, shards - 1, send_sem.at[2])
    take(mean_buf, groups - 1, send_sem.at[3])
    grad_copy.wait()


def solution(mesh):
    groups, shards = mesh.shape["dp"], mesh.shape["tensor"]

    def body(logits, child_ids, leaf_counts, leaf_valid, leaf_temp, leaf_owner):
        pos, cols = logits.shape
        child = child_ids.shape[1]
        cap = pos // groups
        padded = pl.cdiv(cols, WIDE) * WIDE
        vmem = pl.BlockSpec(memory_space=pltpu.VMEM)
        anywhere = pl.BlockSpec(memory_space=pl.ANY)
        gradient, row_loss, mean_loss = pl.pallas_call(
            functools.partial(kernel, groups, shards),
            out_shape=(
                jax.ShapeDtypeStruct((cols, pos), logits.dtype),
                jax.ShapeDtypeStruct((1, pos), F32),
                jax.ShapeDtypeStruct((1, LANES), F32),
            ),
            in_specs=[anywhere] + [vmem] * 5,
            out_specs=(anywhere, vmem, vmem),
            scratch_shapes=[
                pltpu.VMEM((cols, pos), logits.dtype),
                pltpu.VMEM((cols, pos), F32),
                pltpu.VMEM((pos, padded), F32),
                pltpu.VMEM((cols, pos), F32),
                pltpu.VMEM((cols, pos), logits.dtype),
                pltpu.VMEM((groups, cap, 2 * child), F32),
                pltpu.VMEM((groups, cap, 2 * child), F32),
                pltpu.VMEM((pos, 2 * LANES), F32),
                pltpu.VMEM((pos, LANES), jnp.int32),
                pltpu.VMEM((2, pos), F32),
                pltpu.VMEM((shards, 2, pos), F32),
                pltpu.VMEM((1, pos), F32),
                pltpu.VMEM((shards, 1, pos), F32),
                pltpu.VMEM((1, LANES), F32),
                pltpu.VMEM((groups, 1, LANES), F32),
                pltpu.SemaphoreType.DMA,
                pltpu.SemaphoreType.DMA,
                pltpu.SemaphoreType.DMA((4,)),
                pltpu.SemaphoreType.DMA,
                pltpu.SemaphoreType.DMA,
                pltpu.SemaphoreType.DMA,
                pltpu.SemaphoreType.DMA,
            ],
            compiler_params=pltpu.CompilerParams(collective_id=0, has_side_effects=True),
        )(
            logits.T, child_ids.T, leaf_counts.T,
            leaf_valid.reshape(1, pos), leaf_temp.reshape(1, pos), leaf_owner.reshape(1, pos),
        )
        return gradient.T, row_loss.reshape(pos), mean_loss[0, 0]

    return jax.shard_map(
        body,
        mesh=mesh,
        in_specs=(P("dp", "tensor"), P("dp", None), P("dp", None), P("dp"), P("dp"), P("dp")),
        out_specs=(P("dp", "tensor"), P("dp"), P()),
        check_vma=False,
    )
```

```python
import functools

import jax
import jax.numpy as jnp
from jax import lax
from jax.experimental import pallas as pl
from jax.experimental.pallas import tpu as pltpu
from jax.sharding import PartitionSpec as P

MESH = pl.DeviceIdType.MESH
F32 = jnp.float32
BF16 = jnp.bfloat16
LANES = 128
WIDE = 256
CHUNK = 176
HEADS = 24


def dot_nt(lhs, rhs):
    return lax.dot_general(lhs, rhs, (((1,), (1,)), ((), ())), preferred_element_type=F32)


def split(value):
    high = value.astype(BF16)
    rest = value - high.astype(F32)
    middle = rest.astype(BF16)
    return high, middle, (rest - middle.astype(F32)).astype(BF16)


def iota(shape, dim):
    return lax.broadcasted_iota(jnp.int32, shape, dim)


def kernel(
    groups, shards,
    x_hbm, ids_ref, count_ref, valid_ref, temp_ref, owner_ref,
    gout, loss_ref, mean_ref,
    xs, es, dense, turned_x, outbuf, inbuf, head_rows, rest_rows, at_ids, parts,
    stat_send, stat_buf, pick_send, pick_buf, mean_send, mean_buf,
    x_sem, send_sem, route_sem, stat_sem, pick_sem, mean_sem,
):
    cols, pos = x_hbm.shape
    child = ids_ref.shape[0]
    cap = pos // groups
    my_dp = lax.axis_index("dp")
    my_t = lax.axis_index("tensor")
    heads = pl.cdiv(cols, WIDE)

    x_copy = pltpu.make_async_copy(x_hbm, xs.at[pl.ds(0, cols)], x_sem)
    x_copy.start()

    barrier = pltpu.get_barrier_semaphore()

    def greet_dp(k, _):
        pl.semaphore_signal(barrier, inc=1, device_id={"dp": lax.rem(my_dp + k, groups)}, device_id_type=MESH)
        return 0

    def greet_t(k, _):
        pl.semaphore_signal(barrier, inc=1, device_id={"tensor": lax.rem(my_t + k, shards)}, device_id_type=MESH)
        return 0

    lax.fori_loop(1, groups, greet_dp, 0)
    lax.fori_loop(1, shards, greet_t, 0)

    powered = jnp.exp(jnp.log(count_ref[...].astype(F32)) * temp_ref[...])
    weights = jnp.where(iota((child, pos), 0) < valid_ref[...], powered, 0.0)
    share = weights / jnp.sum(weights, axis=0, keepdims=True)
    owner = owner_ref[...]
    shift = pos.bit_length() - 1
    owner_dp = lax.shift_right_logical(owner, shift)
    place = lax.bitwise_and(owner, pos - 1)
    member = jnp.where(iota((groups, pos), 0) == owner_dp, 1.0, 0.0).astype(F32)
    before = jnp.where(iota((pos, pos), 0) < iota((pos, pos), 1), 1.0, 0.0).astype(BF16)
    earlier = jnp.dot(member.astype(BF16), before, preferred_element_type=F32)
    rank = jnp.sum(member * earlier, axis=0, keepdims=True)
    target_row = owner_dp * cap + rank.astype(jnp.int32)
    sender = jnp.where(iota((pos, pos), 0) == target_row, 1.0, 0.0).astype(BF16)
    high, middle, low = split(share)
    place_rows = jnp.broadcast_to(place.astype(F32), (child, pos)).astype(BF16)
    none = jnp.zeros_like(low)
    outgoing = dot_nt(sender, jnp.concatenate([high, place_rows], axis=0))
    outgoing = outgoing + dot_nt(sender, jnp.concatenate([middle, none], axis=0))
    outgoing = outgoing + dot_nt(sender, jnp.concatenate([low, none], axis=0))
    outbuf[...] = outgoing.reshape(groups, cap, 2 * child)

    pairs = pos // 2
    local = ids_ref[...] - my_t * cols
    local = jnp.concatenate([local[:, :pairs], local[:, pairs:]], axis=0)
    local = jnp.transpose(local)
    head = lax.shift_right_arithmetic(local, 8)
    head_rows[...] = jnp.where((head >= 0) & (head < heads), head, -1).astype(F32)
    rest_rows[...] = lax.bitwise_and(local, WIDE - 1).astype(F32)

    x_copy.wait()
    steps = cols // CHUNK

    def part(g):
        return pl.ds(pl.multiple_of(g * CHUNK, CHUNK), CHUNK)

    def fold(value):
        return value.reshape(CHUNK // 8, 8, pos)

    def tops(g, top):
        return jnp.maximum(top, jnp.max(fold(xs[part(g), :].astype(F32)), axis=0))

    top = lax.fori_loop(1, steps, tops, jnp.max(fold(xs[0:CHUNK, :].astype(F32)), axis=0))
    top = jnp.max(top, axis=0, keepdims=True)

    def sums(g, total):
        powers = jnp.exp(xs[part(g), :].astype(F32) - top)
        es[part(g), :] = powers
        return total + jnp.sum(fold(powers), axis=0)

    total = lax.fori_loop(0, steps, sums, jnp.zeros((8, pos), F32))
    own_stats = jnp.concatenate([top, jnp.sum(total, axis=0, keepdims=True)], axis=0)
    stat_send[...] = own_stats
    stat_buf[pl.ds(my_t, 1)] = own_stats.reshape(1, 2, pos)

    pl.semaphore_wait(barrier, groups - 1 + shards - 1)

    def route(k, _):
        peer = lax.rem(my_dp + k, groups)
        pltpu.make_async_remote_copy(
            outbuf.at[peer], inbuf.at[my_dp], send_sem.at[0], route_sem,
            device_id={"dp": peer}, device_id_type=MESH,
        ).start()
        return 0

    def cast(source, buffer, slot, sem, axis, me, count):
        def one(k, _):
            pltpu.make_async_remote_copy(
                source, buffer.at[me], send_sem.at[slot], sem,
                device_id={axis: lax.rem(me + k, count)}, device_id_type=MESH,
            ).start()
            return 0

        lax.fori_loop(1, count, one, 0)

    def take(buffer, count, sem):
        piece = buffer.at[pl.ds(0, count)]
        pltpu.make_async_copy(piece, piece, sem).wait()

    lax.fori_loop(1, groups, route, 0)
    cast(stat_send, stat_buf, 1, stat_sem, "tensor", my_t, shards)
    inbuf[pl.ds(my_dp, 1)] = outbuf[pl.ds(my_dp, 1)]

    xs[cols:, :] = jnp.zeros((xs.shape[0] - cols, pos), xs.dtype)

    def turn(h, _):
        tile = xs[pl.ds(pl.multiple_of(h * WIDE, WIDE), WIDE), :].astype(F32)
        tile = jnp.transpose(tile)
        for c in range(WIDE // LANES):
            turned_x[c, pl.ds(h, pos, stride=HEADS), :] = tile[:, c * LANES : (c + 1) * LANES]
        return 0

    lax.fori_loop(0, heads, turn, 0)

    spread_rows = iota((WIDE, LANES), 0).astype(F32).astype(BF16)
    one = jnp.ones((WIDE, LANES), BF16)
    nil = jnp.zeros((WIDE, LANES), BF16)
    head_index = iota((2 * HEADS, LANES), 0)
    lane = iota((2 * HEADS, LANES), 1)
    second = lane >= child
    head_index = jnp.where(
        second, jnp.where(head_index >= HEADS, head_index - HEADS, -2), jnp.where(head_index < HEADS, head_index, -2)
    ).astype(F32)
    batch = 8

    def pair_onehot(rest, k):
        row = rest[k : k + 1].astype(BF16)
        return jnp.where(spread_rows == row, one, nil)

    def pair_rows(at):
        first = pl.multiple_of(at * HEADS, 8)
        return pl.ds(first, HEADS), pl.ds(pl.multiple_of(first + pairs * HEADS, 8), HEADS)

    def joined(ref, rows):
        return jnp.concatenate([ref[c, rows, :] for c in range(WIDE // LANES)], axis=1)

    def gather(g, _):
        rows = pl.ds(pl.multiple_of(g * batch, batch), batch)
        head, rest = head_rows[rows, :], rest_rows[rows, :]
        found = []
        for k in range(batch):
            upper, lower = pair_rows(g * batch + k)
            values = jnp.concatenate([joined(turned_x, upper), joined(turned_x, lower)], axis=0).astype(BF16)
            reached = jnp.dot(values, pair_onehot(rest, k), preferred_element_type=F32)
            hit = head_index == head[k : k + 1]
            found.append(jnp.sum(jnp.where(hit, reached, 0.0), axis=0, keepdims=True))
        at_ids[rows, :] = jnp.concatenate(found, axis=0)
        return 0

    lax.fori_loop(0, pairs // batch, gather, 0)

    take(inbuf, groups - 1, route_sem)
    turned = jnp.transpose(inbuf[...].reshape(pos, 2 * child))
    label = turned[child : child + 1].astype(jnp.int32)
    receiver = jnp.where(iota((pos, pos), 0) == label, 1.0, 0.0).astype(BF16)
    wanted = [part for part in split(turned[:child]) for _ in range(LANES // child)]
    placed = dot_nt(receiver, jnp.concatenate(wanted, axis=0))
    first_half = iota((pairs, LANES), 1) < child
    target = jnp.zeros((pairs, LANES), F32)
    for k in range(3):
        both = placed[:, k * LANES : (k + 1) * LANES]
        both = jnp.where(first_half, both[:pairs], both[pairs:])
        parts[k] = both
        target = target + both
    product = jnp.transpose(target * at_ids[...])
    own_pick = jnp.concatenate(
        [jnp.sum(product[:child], axis=0, keepdims=True), jnp.sum(product[child:], axis=0, keepdims=True)], axis=1
    )
    pick_send[...] = own_pick
    pick_buf[pl.ds(my_t, 1)] = own_pick.reshape(1, 1, pos)
    cast(pick_send, pick_buf, 2, pick_sem, "tensor", my_t, shards)

    def spread(g, _):
        rows = pl.ds(pl.multiple_of(g * batch, batch), batch)
        head, rest = head_rows[rows, :], rest_rows[rows, :]
        values = [parts[k, rows, :] for k in range(3)]
        for k in range(batch):
            hit = head_index == head[k : k + 1]
            chosen = jnp.concatenate([jnp.where(hit, value[k : k + 1], 0.0) for value in values], axis=0)
            found = dot_nt(chosen.astype(BF16), pair_onehot(rest, k))
            size = 2 * HEADS
            found = found[:size] + found[size : 2 * size] + found[2 * size :]
            upper, lower = pair_rows(g * batch + k)
            for c in range(WIDE // LANES):
                dense[c, upper, :] = found[:HEADS, c * LANES : (c + 1) * LANES]
                dense[c, lower, :] = found[HEADS:, c * LANES : (c + 1) * LANES]
        return 0

    lax.fori_loop(0, pairs // batch, spread, 0)

    take(stat_buf, shards - 1, stat_sem)
    every_top, every_sum = stat_buf[:, 0, :], stat_buf[:, 1, :]
    peak = jnp.max(every_top, axis=0, keepdims=True)
    whole_sum = jnp.sum(every_sum * jnp.exp(every_top - peak), axis=0, keepdims=True)
    scale = jnp.exp(top - peak) / whole_sum

    def gradient(h, rows, size):
        tile = jnp.transpose(joined(dense, pl.ds(h, pos, stride=HEADS)))[:size]
        gout[rows, :] = (es[rows, :] * scale - tile).astype(gout.dtype)

    def gradient_step(h, _):
        gradient(h, pl.ds(pl.multiple_of(h * WIDE, WIDE), WIDE), WIDE)
        return 0

    whole = cols // WIDE
    lax.fori_loop(0, whole, gradient_step, 0)
    if cols > whole * WIDE:
        gradient(whole, pl.ds(whole * WIDE, cols - whole * WIDE), cols - whole * WIDE)

    take(pick_buf, shards - 1, pick_sem)
    loss = peak + jnp.log(whole_sum) - jnp.sum(pick_buf[...], axis=0)
    loss_ref[...] = loss
    own_mean = jnp.broadcast_to(jnp.sum(loss, axis=1, keepdims=True), (1, LANES))
    mean_send[...] = own_mean
    mean_buf[pl.ds(my_dp, 1)] = own_mean.reshape(1, 1, LANES)
    cast(mean_send, mean_buf, 3, mean_sem, "dp", my_dp, groups)
    take(mean_buf, groups - 1, mean_sem)
    mean_ref[...] = jnp.sum(mean_buf[...], axis=0) / (groups * pos)

    take(outbuf, groups - 1, send_sem.at[0])
    take(stat_buf, shards - 1, send_sem.at[1])
    take(pick_buf, shards - 1, send_sem.at[2])
    take(mean_buf, groups - 1, send_sem.at[3])


def solution(mesh):
    groups, shards = mesh.shape["dp"], mesh.shape["tensor"]

    def body(logits, child_ids, leaf_counts, leaf_valid, leaf_temp, leaf_owner):
        pos, cols = logits.shape
        child = child_ids.shape[1]
        cap = pos // groups
        padded = pl.cdiv(cols, WIDE) * WIDE
        vmem = pl.BlockSpec(memory_space=pltpu.VMEM)
        anywhere = pl.BlockSpec(memory_space=pl.ANY)
        gradient, row_loss, mean_loss = pl.pallas_call(
            functools.partial(kernel, groups, shards),
            out_shape=(
                pltpu.VMEM((cols, pos), logits.dtype),
                pltpu.VMEM((1, pos), F32),
                pltpu.VMEM((1, LANES), F32),
            ),
            in_specs=[anywhere] + [vmem] * 5,
            out_specs=(vmem, vmem, vmem),
            scratch_shapes=[
                pltpu.VMEM((padded, pos), logits.dtype),
                pltpu.VMEM((cols, pos), F32),
                pltpu.VMEM((WIDE // LANES, pos * HEADS, LANES), F32),
                pltpu.VMEM((WIDE // LANES, pos * HEADS, LANES), F32),
                pltpu.VMEM((groups, cap, 2 * child), F32),
                pltpu.VMEM((groups, cap, 2 * child), F32),
                pltpu.VMEM((pos // 2, LANES), F32),
                pltpu.VMEM((pos // 2, LANES), F32),
                pltpu.VMEM((pos // 2, LANES), F32),
                pltpu.VMEM((3, pos // 2, LANES), F32),
                pltpu.VMEM((2, pos), F32),
                pltpu.VMEM((shards, 2, pos), F32),
                pltpu.VMEM((1, pos), F32),
                pltpu.VMEM((shards, 1, pos), F32),
                pltpu.VMEM((1, LANES), F32),
                pltpu.VMEM((groups, 1, LANES), F32),
                pltpu.SemaphoreType.DMA,
                pltpu.SemaphoreType.DMA((4,)),
                pltpu.SemaphoreType.DMA,
                pltpu.SemaphoreType.DMA,
                pltpu.SemaphoreType.DMA,
                pltpu.SemaphoreType.DMA,
            ],
            compiler_params=pltpu.CompilerParams(collective_id=0, has_side_effects=True),
        )(
            logits.T, child_ids.T, leaf_counts.T,
            leaf_valid.reshape(1, pos), leaf_temp.reshape(1, pos), leaf_owner.reshape(1, pos),
        )
        return gradient.T, row_loss.reshape(pos), mean_loss[0, 0]

    return jax.shard_map(
        body,
        mesh=mesh,
        in_specs=(P("dp", "tensor"), P("dp", None), P("dp", None), P("dp"), P("dp"), P("dp")),
        out_specs=(P("dp", "tensor"), P("dp"), P()),
        check_vma=False,
    )
```

```python
import functools

import jax
import jax.numpy as jnp
from jax import lax
from jax.experimental import pallas as pl
from jax.experimental.pallas import tpu as pltpu
from jax.sharding import PartitionSpec as P

MESH = pl.DeviceIdType.MESH
F32 = jnp.float32
BF16 = jnp.bfloat16
LANES = 128
WIDE = 256
CHUNK = 176
HEADS = 24


def dot_nt(lhs, rhs):
    return lax.dot_general(lhs, rhs, (((1,), (1,)), ((), ())), preferred_element_type=F32)


def split(value):
    high = value.astype(BF16)
    rest = value - high.astype(F32)
    middle = rest.astype(BF16)
    return high, middle, (rest - middle.astype(F32)).astype(BF16)


def from_afar(step, count):
    away = lax.div(step + 1, 2)
    return count // 2 + jnp.where(lax.rem(step, 2) == 0, -away, away)


def repeat(count, factor, step):
    def trip(g, _):
        for k in range(factor):
            step(g * factor + k)
        return 0

    lax.fori_loop(0, count // factor, trip, 0)
    for k in range(count // factor * factor, count):
        step(k)


def iota(shape, dim):
    return lax.broadcasted_iota(jnp.int32, shape, dim)


def kernel(
    groups, shards,
    x_hbm, ids_ref, count_ref, valid_ref, temp_ref, owner_ref,
    gout, loss_ref, mean_ref,
    xs, es, dense, turned_x, outbuf, inbuf, head_rows, rest_rows, at_ids, parts,
    stat_send, stat_buf, mean_send, mean_buf,
    x_sem, send_sem, route_sem, stat_sem, mean_sem,
):
    cols, pos = x_hbm.shape
    child = ids_ref.shape[0]
    cap = pos // groups
    my_dp = lax.axis_index("dp")
    my_t = lax.axis_index("tensor")
    heads = pl.cdiv(cols, WIDE)

    x_copy = pltpu.make_async_copy(x_hbm, xs.at[pl.ds(0, cols)], x_sem)
    x_copy.start()

    barrier = pltpu.get_barrier_semaphore()

    def peer_of(me, k, count):
        return lax.rem(me + from_afar(k, count), count)

    def greet_t(k, _):
        pl.semaphore_signal(barrier, inc=1, device_id={"tensor": peer_of(my_t, k, shards)}, device_id_type=MESH)
        return 0

    def greet_dp(k, _):
        pl.semaphore_signal(barrier, inc=1, device_id={"dp": peer_of(my_dp, k, groups)}, device_id_type=MESH)
        return 0

    lax.fori_loop(0, shards - 1, greet_t, 0)
    lax.fori_loop(0, groups - 1, greet_dp, 0)

    powered = jnp.exp(jnp.log(count_ref[...].astype(F32)) * temp_ref[...])
    weights = jnp.where(iota((child, pos), 0) < valid_ref[...], powered, 0.0)
    share = weights / jnp.sum(weights, axis=0, keepdims=True)
    owner = owner_ref[...]
    shift = pos.bit_length() - 1
    owner_dp = lax.shift_right_logical(owner, shift)
    place = lax.bitwise_and(owner, pos - 1)
    member = jnp.where(iota((groups, pos), 0) == owner_dp, 1.0, 0.0).astype(F32)
    before = jnp.where(iota((pos, pos), 0) < iota((pos, pos), 1), 1.0, 0.0).astype(BF16)
    earlier = jnp.dot(member.astype(BF16), before, preferred_element_type=F32)
    rank = jnp.sum(member * earlier, axis=0, keepdims=True)
    target_row = owner_dp * cap + rank.astype(jnp.int32)
    sender = jnp.where(iota((pos, pos), 0) == target_row, 1.0, 0.0).astype(BF16)
    high, middle, low = split(share)
    place_rows = jnp.broadcast_to(place.astype(F32), (child, pos)).astype(BF16)
    none = jnp.zeros_like(low)
    outgoing = dot_nt(sender, jnp.concatenate([high, place_rows], axis=0))
    outgoing = outgoing + dot_nt(sender, jnp.concatenate([middle, none], axis=0))
    outgoing = outgoing + dot_nt(sender, jnp.concatenate([low, none], axis=0))
    outbuf[...] = outgoing.reshape(groups, cap, 2 * child)

    pairs = pos // 2
    local = ids_ref[...] - my_t * cols
    local = jnp.concatenate([local[:, :pairs], local[:, pairs:]], axis=0)
    local = jnp.transpose(local)
    head = lax.shift_right_arithmetic(local, 8)
    head_rows[...] = jnp.where((head >= 0) & (head < heads), head, -1).astype(F32)
    rest_rows[...] = lax.bitwise_and(local, WIDE - 1).astype(F32)

    x_copy.wait()
    steps = cols // CHUNK

    def part(g):
        return pl.ds(pl.multiple_of(g * CHUNK, CHUNK), CHUNK)

    def fold(value):
        return value.reshape(CHUNK // 8, 8, pos)

    def tops(g, top):
        return jnp.maximum(top, jnp.max(fold(xs[part(g), :].astype(F32)), axis=0))

    top = lax.fori_loop(1, steps, tops, jnp.max(fold(xs[0:CHUNK, :].astype(F32)), axis=0))
    top = jnp.max(top, axis=0, keepdims=True)

    def sums(g, total):
        powers = jnp.exp(xs[part(g), :].astype(F32) - top)
        es[part(g), :] = powers
        return total + jnp.sum(fold(powers), axis=0)

    total = lax.fori_loop(0, steps, sums, jnp.zeros((8, pos), F32))
    own_sum = jnp.sum(total, axis=0, keepdims=True)

    xs[cols:, :] = jnp.zeros((xs.shape[0] - cols, pos), xs.dtype)

    def turn(h):
        at = h * WIDE if isinstance(h, int) else pl.multiple_of(h * WIDE, WIDE)
        tile = jnp.transpose(xs[pl.ds(at, WIDE), :]).astype(F32)
        for c in range(WIDE // LANES):
            turned_x[c, pl.ds(h, pos, stride=HEADS), :] = tile[:, c * LANES : (c + 1) * LANES]

    repeat(heads, 3, turn)

    pl.semaphore_wait(barrier, groups - 1 + shards - 1)

    def route(k, _):
        peer = peer_of(my_dp, k, groups)
        pltpu.make_async_remote_copy(
            outbuf.at[peer], inbuf.at[my_dp], send_sem.at[0], route_sem,
            device_id={"dp": peer}, device_id_type=MESH,
        ).start()
        return 0

    def cast(source, buffer, slot, sem, axis, me, count):
        def one(k, _):
            pltpu.make_async_remote_copy(
                source, buffer.at[me], send_sem.at[slot], sem,
                device_id={axis: peer_of(me, k, count)}, device_id_type=MESH,
            ).start()
            return 0

        lax.fori_loop(0, count - 1, one, 0)

    def take(buffer, count, sem):
        piece = buffer.at[pl.ds(0, count)]
        pltpu.make_async_copy(piece, piece, sem).wait()

    lax.fori_loop(0, groups - 1, route, 0)
    inbuf[pl.ds(my_dp, 1)] = outbuf[pl.ds(my_dp, 1)]

    spread_rows = iota((WIDE, LANES), 0).astype(F32).astype(BF16)
    one = jnp.ones((WIDE, LANES), BF16)
    nil = jnp.zeros((WIDE, LANES), BF16)
    head_index = iota((2 * HEADS, LANES), 0)
    lane = iota((2 * HEADS, LANES), 1)
    second = lane >= child
    head_index = jnp.where(
        second, jnp.where(head_index >= HEADS, head_index - HEADS, -2), jnp.where(head_index < HEADS, head_index, -2)
    ).astype(F32)
    batch = 8

    def pair_onehot(rest, k):
        row = rest[k : k + 1].astype(BF16)
        return jnp.where(spread_rows == row, one, nil)

    def pair_rows(at):
        first = pl.multiple_of(at * HEADS, 8)
        return pl.ds(first, HEADS), pl.ds(pl.multiple_of(first + pairs * HEADS, 8), HEADS)

    def joined(ref, rows):
        return jnp.concatenate([ref[c, rows, :] for c in range(WIDE // LANES)], axis=1)

    def gather(g):
        rows = pl.ds(pl.multiple_of(g * batch, batch), batch)
        head, rest = head_rows[rows, :], rest_rows[rows, :]
        found = []
        for k in range(batch):
            upper, lower = pair_rows(g * batch + k)
            values = jnp.concatenate([joined(turned_x, upper), joined(turned_x, lower)], axis=0).astype(BF16)
            reached = jnp.dot(values, pair_onehot(rest, k), preferred_element_type=F32)
            hit = head_index == head[k : k + 1]
            found.append(jnp.sum(jnp.where(hit, reached, 0.0), axis=0, keepdims=True))
        at_ids[rows, :] = jnp.concatenate(found, axis=0)

    repeat(pairs // batch, 8, gather)

    take(inbuf, groups - 1, route_sem)
    turned = jnp.transpose(inbuf[...].reshape(pos, 2 * child))
    label = turned[child : child + 1].astype(jnp.int32)
    receiver = jnp.where(iota((pos, pos), 0) == label, 1.0, 0.0).astype(BF16)
    wanted = [part for part in split(turned[:child]) for _ in range(LANES // child)]
    placed = dot_nt(receiver, jnp.concatenate(wanted, axis=0))
    first_half = iota((pairs, LANES), 1) < child
    target = jnp.zeros((pairs, LANES), F32)
    for k in range(3):
        both = placed[:, k * LANES : (k + 1) * LANES]
        both = jnp.where(first_half, both[:pairs], both[pairs:])
        parts[k] = both
        target = target + both
    product = jnp.transpose(target * at_ids[...])
    own_pick = jnp.concatenate(
        [jnp.sum(product[:child], axis=0, keepdims=True), jnp.sum(product[child:], axis=0, keepdims=True)], axis=1
    )
    own_stats = jnp.concatenate([top, own_sum, own_pick], axis=0)
    stat_send[...] = own_stats
    stat_buf[pl.ds(my_t, 1)] = own_stats.reshape(1, 3, pos)
    cast(stat_send, stat_buf, 1, stat_sem, "tensor", my_t, shards)

    def spread(g):
        rows = pl.ds(pl.multiple_of(g * batch, batch), batch)
        head, rest = head_rows[rows, :], rest_rows[rows, :]
        values = [parts[k, rows, :] for k in range(3)]
        for k in range(batch):
            hit = head_index == head[k : k + 1]
            chosen = jnp.concatenate([jnp.where(hit, value[k : k + 1], 0.0) for value in values], axis=0)
            found = dot_nt(chosen.astype(BF16), pair_onehot(rest, k))
            size = 2 * HEADS
            found = found[:size] + found[size : 2 * size] + found[2 * size :]
            upper, lower = pair_rows(g * batch + k)
            for c in range(WIDE // LANES):
                dense[c, upper, :] = found[:HEADS, c * LANES : (c + 1) * LANES]
                dense[c, lower, :] = found[HEADS:, c * LANES : (c + 1) * LANES]

    repeat(pairs // batch, 4, spread)

    take(stat_buf, shards - 1, stat_sem)
    every_top, every_sum = stat_buf[:, 0, :], stat_buf[:, 1, :]
    peak = jnp.max(every_top, axis=0, keepdims=True)
    whole_sum = jnp.sum(every_sum * jnp.exp(every_top - peak), axis=0, keepdims=True)
    loss = peak + jnp.log(whole_sum) - jnp.sum(stat_buf[:, 2, :], axis=0, keepdims=True)
    loss_ref[...] = loss
    own_mean = jnp.broadcast_to(jnp.sum(loss, axis=1, keepdims=True), (1, LANES))
    mean_send[...] = own_mean
    mean_buf[pl.ds(my_dp, 1)] = own_mean.reshape(1, 1, LANES)
    cast(mean_send, mean_buf, 2, mean_sem, "dp", my_dp, groups)

    scale = jnp.exp(top - peak) / whole_sum

    def gradient(h, size=WIDE):
        at = h * WIDE if isinstance(h, int) else pl.multiple_of(h * WIDE, WIDE)
        rows = pl.ds(at, size)
        tile = jnp.transpose(joined(dense, pl.ds(h, pos, stride=HEADS)))[:size]
        gout[rows, :] = (es[rows, :] * scale - tile).astype(gout.dtype)

    whole = cols // WIDE
    repeat(whole, 6, gradient)
    if cols > whole * WIDE:
        gradient(whole, cols - whole * WIDE)

    take(mean_buf, groups - 1, mean_sem)
    mean_ref[...] = jnp.sum(mean_buf[...], axis=0) / (groups * pos)

    take(outbuf, groups - 1, send_sem.at[0])
    take(stat_buf, shards - 1, send_sem.at[1])
    take(mean_buf, groups - 1, send_sem.at[2])


def solution(mesh):
    groups, shards = mesh.shape["dp"], mesh.shape["tensor"]

    def body(logits, child_ids, leaf_counts, leaf_valid, leaf_temp, leaf_owner):
        pos, cols = logits.shape
        child = child_ids.shape[1]
        cap = pos // groups
        padded = pl.cdiv(cols, WIDE) * WIDE
        vmem = pl.BlockSpec(memory_space=pltpu.VMEM)
        anywhere = pl.BlockSpec(memory_space=pl.ANY)
        gradient, row_loss, mean_loss = pl.pallas_call(
            functools.partial(kernel, groups, shards),
            out_shape=(
                pltpu.VMEM((cols, pos), logits.dtype),
                pltpu.VMEM((1, pos), F32),
                pltpu.VMEM((1, LANES), F32),
            ),
            in_specs=[anywhere] + [vmem] * 5,
            out_specs=(vmem, vmem, vmem),
            scratch_shapes=[
                pltpu.VMEM((padded, pos), logits.dtype),
                pltpu.VMEM((cols, pos), F32),
                pltpu.VMEM((WIDE // LANES, pos * HEADS, LANES), F32),
                pltpu.VMEM((WIDE // LANES, pos * HEADS, LANES), F32),
                pltpu.VMEM((groups, cap, 2 * child), F32),
                pltpu.VMEM((groups, cap, 2 * child), F32),
                pltpu.VMEM((pos // 2, LANES), F32),
                pltpu.VMEM((pos // 2, LANES), F32),
                pltpu.VMEM((pos // 2, LANES), F32),
                pltpu.VMEM((3, pos // 2, LANES), F32),
                pltpu.VMEM((3, pos), F32),
                pltpu.VMEM((shards, 3, pos), F32),
                pltpu.VMEM((1, LANES), F32),
                pltpu.VMEM((groups, 1, LANES), F32),
                pltpu.SemaphoreType.DMA,
                pltpu.SemaphoreType.DMA((3,)),
                pltpu.SemaphoreType.DMA,
                pltpu.SemaphoreType.DMA,
                pltpu.SemaphoreType.DMA,
            ],
            compiler_params=pltpu.CompilerParams(collective_id=0, has_side_effects=True),
        )(
            logits.T, child_ids.T, leaf_counts.T,
            leaf_valid.reshape(1, pos), leaf_temp.reshape(1, pos), leaf_owner.reshape(1, pos),
        )
        return gradient.T, row_loss.reshape(pos), mean_loss[0, 0]

    return jax.shard_map(
        body,
        mesh=mesh,
        in_specs=(P("dp", "tensor"), P("dp", None), P("dp", None), P("dp"), P("dp"), P("dp")),
        out_specs=(P("dp", "tensor"), P("dp"), P()),
        check_vma=False,
    )
```

```python
import functools

import jax
import jax.numpy as jnp
from jax import lax
from jax.experimental import pallas as pl
from jax.experimental.pallas import tpu as pltpu
from jax.sharding import PartitionSpec as P

MESH = pl.DeviceIdType.MESH
F32 = jnp.float32
BF16 = jnp.bfloat16
LANES = 128
WIDE = 256
CHUNK = 176
HEADS = 24


def dot_nt(lhs, rhs):
    return lax.dot_general(lhs, rhs, (((1,), (1,)), ((), ())), preferred_element_type=F32)


def split(value):
    high = value.astype(BF16)
    rest = value - high.astype(F32)
    middle = rest.astype(BF16)
    return high, middle, (rest - middle.astype(F32)).astype(BF16)


def offsets(count):
    return sorted(range(1, count), key=lambda k: -min(k, count - k))


def near_offsets(count):
    return [k for k in offsets(count) if min(k, count - k) <= count // 4 + 1]


def repeat(count, factor, step):
    def trip(g, _):
        for k in range(factor):
            step(g * factor + k)
        return 0

    lax.fori_loop(0, count // factor, trip, 0)
    for k in range(count // factor * factor, count):
        step(k)


def iota(shape, dim):
    return lax.broadcasted_iota(jnp.int32, shape, dim)


def kernel(
    groups, shards,
    x_hbm, ids_ref, count_ref, valid_ref, temp_ref, owner_ref,
    gout, loss_ref, mean_ref,
    xs, es, dense, turned_x, outbuf, inbuf, head_rows, rest_rows, at_ids, parts,
    stat_send, stat_buf, mean_send, mean_buf,
    x_sem, send_sem, route_sem, stat_sem, mean_sem, hello_sem,
):
    cols, pos = x_hbm.shape
    child = ids_ref.shape[0]
    cap = pos // groups
    my_dp = lax.axis_index("dp")
    my_t = lax.axis_index("tensor")
    heads = pl.cdiv(cols, WIDE)

    x_copy = pltpu.make_async_copy(x_hbm, xs.at[pl.ds(0, cols)], x_sem)
    x_copy.start()

    barrier = pltpu.get_barrier_semaphore()

    def peer_of(me, k, count):
        return lax.rem(me + k, count)

    near = near_offsets(shards)
    for k in near:
        pl.semaphore_signal(barrier, inc=1, device_id={"tensor": peer_of(my_t, k, shards)}, device_id_type=MESH)
    for k in offsets(groups):
        pl.semaphore_signal(barrier, inc=1, device_id={"dp": peer_of(my_dp, k, groups)}, device_id_type=MESH)

    powered = jnp.exp(jnp.log(count_ref[...].astype(F32)) * temp_ref[...])
    weights = jnp.where(iota((child, pos), 0) < valid_ref[...], powered, 0.0)
    share = weights / jnp.sum(weights, axis=0, keepdims=True)
    owner = owner_ref[...]
    shift = pos.bit_length() - 1
    owner_dp = lax.shift_right_logical(owner, shift)
    place = lax.bitwise_and(owner, pos - 1)
    member = jnp.where(iota((groups, pos), 0) == owner_dp, 1.0, 0.0).astype(F32)
    before = jnp.where(iota((pos, pos), 0) < iota((pos, pos), 1), 1.0, 0.0).astype(BF16)
    earlier = jnp.dot(member.astype(BF16), before, preferred_element_type=F32)
    rank = jnp.sum(member * earlier, axis=0, keepdims=True)
    target_row = owner_dp * cap + rank.astype(jnp.int32)
    sender = jnp.where(iota((pos, pos), 0) == target_row, 1.0, 0.0).astype(BF16)
    high, middle, low = split(share)
    place_rows = jnp.broadcast_to(place.astype(F32), (child, pos)).astype(BF16)
    none = jnp.zeros_like(low)
    outgoing = dot_nt(sender, jnp.concatenate([high, place_rows], axis=0))
    outgoing = outgoing + dot_nt(sender, jnp.concatenate([middle, none], axis=0))
    outgoing = outgoing + dot_nt(sender, jnp.concatenate([low, none], axis=0))
    outbuf[...] = outgoing.reshape(groups, cap, 2 * child)

    pairs = pos // 2
    local = ids_ref[...] - my_t * cols
    local = jnp.concatenate([local[:, :pairs], local[:, pairs:]], axis=0)
    local = jnp.transpose(local)
    head = lax.shift_right_arithmetic(local, 8)
    head_rows[...] = jnp.where((head >= 0) & (head < heads), head, -1).astype(F32)
    rest_rows[...] = lax.bitwise_and(local, WIDE - 1).astype(F32)

    x_copy.wait()
    steps = cols // CHUNK

    def part(g):
        return pl.ds(pl.multiple_of(g * CHUNK, CHUNK), CHUNK)

    def fold(value):
        return value.reshape(CHUNK // 8, 8, pos)

    def peaks(values):
        return jnp.max(values.reshape(CHUNK // 16, 16, pos), axis=0)

    def tops(g, top):
        return jnp.maximum(top, peaks(xs[part(g), :]))

    top = lax.fori_loop(1, steps, tops, peaks(xs[0:CHUNK, :]))
    top = jnp.max(top.astype(F32), axis=0, keepdims=True)

    def sums(g, total):
        powers = jnp.exp(xs[part(g), :].astype(F32) - top)
        es[part(g), :] = powers
        return total + jnp.sum(fold(powers), axis=0)

    total = lax.fori_loop(0, steps, sums, jnp.zeros((8, pos), F32))
    own_sum = jnp.sum(total, axis=0, keepdims=True)

    pl.semaphore_wait(barrier, groups - 1 + len(near))

    def cast(source, buffer, slot, sem, axis, me, count):
        for k in offsets(count):
            pltpu.make_async_remote_copy(
                source, buffer.at[me], send_sem.at[slot], sem,
                device_id={axis: peer_of(me, k, count)}, device_id_type=MESH,
            ).start()

    def take(buffer, count, sem):
        piece = buffer.at[pl.ds(0, count)]
        pltpu.make_async_copy(piece, piece, sem).wait()

    for k in offsets(groups):
        peer = peer_of(my_dp, k, groups)
        pltpu.make_async_remote_copy(
            outbuf.at[peer], inbuf.at[my_dp], send_sem.at[0], route_sem,
            device_id={"dp": peer}, device_id_type=MESH,
        ).start()
    for k in near:
        pl.semaphore_signal(hello_sem, inc=1, device_id={"tensor": peer_of(my_t, k, shards)}, device_id_type=MESH)
    inbuf[pl.ds(my_dp, 1)] = outbuf[pl.ds(my_dp, 1)]

    xs[cols:, :] = jnp.zeros((xs.shape[0] - cols, pos), xs.dtype)

    def turn(h):
        at = h * WIDE if isinstance(h, int) else pl.multiple_of(h * WIDE, WIDE)
        tile = jnp.transpose(xs[pl.ds(at, WIDE), :]).astype(F32)
        for c in range(WIDE // LANES):
            turned_x[c, pl.ds(h, pos, stride=HEADS), :] = tile[:, c * LANES : (c + 1) * LANES]

    repeat(heads, 3, turn)

    spread_rows = iota((WIDE, LANES), 0).astype(F32).astype(BF16)
    one = jnp.ones((WIDE, LANES), BF16)
    nil = jnp.zeros((WIDE, LANES), BF16)
    head_index = iota((2 * HEADS, LANES), 0)
    lane = iota((2 * HEADS, LANES), 1)
    second = lane >= child
    head_index = jnp.where(
        second, jnp.where(head_index >= HEADS, head_index - HEADS, -2), jnp.where(head_index < HEADS, head_index, -2)
    ).astype(F32)
    batch = 8

    def pair_onehot(rest, k):
        row = rest[k : k + 1].astype(BF16)
        return jnp.where(spread_rows == row, one, nil)

    def pair_rows(at):
        first = pl.multiple_of(at * HEADS, 8)
        return pl.ds(first, HEADS), pl.ds(pl.multiple_of(first + pairs * HEADS, 8), HEADS)

    def joined(ref, rows):
        return jnp.concatenate([ref[c, rows, :] for c in range(WIDE // LANES)], axis=1)

    def gather(g):
        rows = pl.ds(pl.multiple_of(g * batch, batch), batch)
        head, rest = head_rows[rows, :], rest_rows[rows, :]
        found = []
        for k in range(batch):
            upper, lower = pair_rows(g * batch + k)
            values = jnp.concatenate([joined(turned_x, upper), joined(turned_x, lower)], axis=0).astype(BF16)
            reached = jnp.dot(values, pair_onehot(rest, k), preferred_element_type=F32)
            hit = head_index == head[k : k + 1]
            found.append(jnp.sum(jnp.where(hit, reached, 0.0), axis=0, keepdims=True))
        at_ids[rows, :] = jnp.concatenate(found, axis=0)

    repeat(pairs // batch, 8, gather)

    take(inbuf, groups - 1, route_sem)
    turned = jnp.transpose(inbuf[...].reshape(pos, 2 * child))
    label = turned[child : child + 1].astype(jnp.int32)
    receiver = jnp.where(iota((pos, pos), 0) == label, 1.0, 0.0).astype(BF16)
    wanted = [part for part in split(turned[:child]) for _ in range(LANES // child)]
    placed = dot_nt(receiver, jnp.concatenate(wanted, axis=0))
    first_half = iota((pairs, LANES), 1) < child
    target = jnp.zeros((pairs, LANES), F32)
    for k in range(3):
        both = placed[:, k * LANES : (k + 1) * LANES]
        both = jnp.where(first_half, both[:pairs], both[pairs:])
        parts[k] = both
        target = target + both
    product = jnp.transpose(target * at_ids[...])
    own_pick = jnp.concatenate(
        [jnp.sum(product[:child], axis=0, keepdims=True), jnp.sum(product[child:], axis=0, keepdims=True)], axis=1
    )
    own_stats = jnp.concatenate([top, own_sum, own_pick], axis=0)
    stat_send[...] = own_stats
    stat_buf[pl.ds(my_t, 1)] = own_stats.reshape(1, 3, pos)
    pl.semaphore_wait(hello_sem, len(near))
    cast(stat_send, stat_buf, 1, stat_sem, "tensor", my_t, shards)

    def spread(g):
        rows = pl.ds(pl.multiple_of(g * batch, batch), batch)
        head, rest = head_rows[rows, :], rest_rows[rows, :]
        values = [parts[k, rows, :] for k in range(3)]
        for k in range(batch):
            hit = head_index == head[k : k + 1]
            chosen = jnp.concatenate([jnp.where(hit, value[k : k + 1], 0.0) for value in values], axis=0)
            found = dot_nt(chosen.astype(BF16), pair_onehot(rest, k))
            size = 2 * HEADS
            found = found[:size] + found[size : 2 * size] + found[2 * size :]
            upper, lower = pair_rows(g * batch + k)
            for c in range(WIDE // LANES):
                dense[c, upper, :] = found[:HEADS, c * LANES : (c + 1) * LANES]
                dense[c, lower, :] = found[HEADS:, c * LANES : (c + 1) * LANES]

    repeat(pairs // batch, 4, spread)

    take(stat_buf, shards - 1, stat_sem)
    every_top, every_sum = stat_buf[:, 0, :], stat_buf[:, 1, :]
    peak = jnp.max(every_top, axis=0, keepdims=True)
    whole_sum = jnp.sum(every_sum * jnp.exp(every_top - peak), axis=0, keepdims=True)
    loss = peak + jnp.log(whole_sum) - jnp.sum(stat_buf[:, 2, :], axis=0, keepdims=True)
    loss_ref[...] = loss
    own_mean = jnp.broadcast_to(jnp.sum(loss, axis=1, keepdims=True), (1, LANES))
    mean_send[...] = own_mean
    mean_buf[pl.ds(my_dp, 1)] = own_mean.reshape(1, 1, LANES)
    cast(mean_send, mean_buf, 2, mean_sem, "dp", my_dp, groups)

    scale = jnp.exp(top - peak) / whole_sum

    def gradient(h, size=WIDE):
        at = h * WIDE if isinstance(h, int) else pl.multiple_of(h * WIDE, WIDE)
        rows = pl.ds(at, size)
        tile = jnp.transpose(joined(dense, pl.ds(h, pos, stride=HEADS)))[:size]
        gout[rows, :] = (es[rows, :] * scale - tile).astype(gout.dtype)

    whole = cols // WIDE
    repeat(whole, 6, gradient)
    if cols > whole * WIDE:
        gradient(whole, cols - whole * WIDE)

    take(mean_buf, groups - 1, mean_sem)
    mean_ref[...] = jnp.sum(mean_buf[...], axis=0) / (groups * pos)

    take(outbuf, groups - 1, send_sem.at[0])
    take(stat_buf, shards - 1, send_sem.at[1])
    take(mean_buf, groups - 1, send_sem.at[2])


def leave(*refs):
    count = len(refs) // 2
    sems = refs[-1]
    copies = [pltpu.make_async_copy(refs[k], refs[count + k], sems.at[k]) for k in range(count)]
    for copy in copies:
        copy.start()
    for copy in copies:
        copy.wait()


def solution(mesh):
    groups, shards = mesh.shape["dp"], mesh.shape["tensor"]

    def body(logits, child_ids, leaf_counts, leaf_valid, leaf_temp, leaf_owner):
        pos, cols = logits.shape
        child = child_ids.shape[1]
        cap = pos // groups
        padded = pl.cdiv(cols, WIDE) * WIDE
        vmem = pl.BlockSpec(memory_space=pltpu.VMEM)
        anywhere = pl.BlockSpec(memory_space=pl.ANY)
        results = pl.pallas_call(
            functools.partial(kernel, groups, shards),
            out_shape=(
                pltpu.VMEM((cols, pos), logits.dtype),
                pltpu.VMEM((1, pos), F32),
                pltpu.VMEM((1, LANES), F32),
            ),
            in_specs=[anywhere] + [vmem] * 5,
            out_specs=(vmem, vmem, vmem),
            scratch_shapes=[
                pltpu.VMEM((padded, pos), logits.dtype),
                pltpu.VMEM((cols, pos), F32),
                pltpu.VMEM((WIDE // LANES, pos * HEADS, LANES), F32),
                pltpu.VMEM((WIDE // LANES, pos * HEADS, LANES), F32),
                pltpu.VMEM((groups, cap, 2 * child), F32),
                pltpu.VMEM((groups, cap, 2 * child), F32),
                pltpu.VMEM((pos // 2, LANES), F32),
                pltpu.VMEM((pos // 2, LANES), F32),
                pltpu.VMEM((pos // 2, LANES), F32),
                pltpu.VMEM((3, pos // 2, LANES), F32),
                pltpu.VMEM((3, pos), F32),
                pltpu.VMEM((shards, 3, pos), F32),
                pltpu.VMEM((1, LANES), F32),
                pltpu.VMEM((groups, 1, LANES), F32),
                pltpu.SemaphoreType.DMA,
                pltpu.SemaphoreType.DMA((3,)),
                pltpu.SemaphoreType.DMA,
                pltpu.SemaphoreType.DMA,
                pltpu.SemaphoreType.DMA,
                pltpu.SemaphoreType.REGULAR,
            ],
            compiler_params=pltpu.CompilerParams(collective_id=0, has_side_effects=True),
        )(
            logits.T, child_ids.T, leaf_counts.T,
            leaf_valid.reshape(1, pos), leaf_temp.reshape(1, pos), leaf_owner.reshape(1, pos),
        )
        gradient, row_loss, mean_loss = pl.pallas_call(
            leave,
            out_shape=[jax.ShapeDtypeStruct(value.shape, value.dtype) for value in results],
            in_specs=[vmem] * 3,
            out_specs=[anywhere] * 3,
            scratch_shapes=[pltpu.SemaphoreType.DMA((3,))],
        )(*(pltpu.with_memory_space_constraint(value, pltpu.VMEM) for value in results))
        return gradient.T, row_loss.reshape(pos), mean_loss[0, 0]

    return jax.shard_map(
        body,
        mesh=mesh,
        in_specs=(P("dp", "tensor"), P("dp", None), P("dp", None), P("dp"), P("dp"), P("dp")),
        out_specs=(P("dp", "tensor"), P("dp"), P()),
        check_vma=False,
    )
```

```python
import functools

import jax
import jax.numpy as jnp
from jax import lax
from jax.experimental import pallas as pl
from jax.experimental.pallas import tpu as pltpu
from jax.sharding import PartitionSpec as P

MESH = pl.DeviceIdType.MESH
F32 = jnp.float32
BF16 = jnp.bfloat16
LANES = 128
WIDE = 256
CHUNK = 176
HEADS = 24


def dot_nt(lhs, rhs):
    return lax.dot_general(lhs, rhs, (((1,), (1,)), ((), ())), preferred_element_type=F32)


def split(value):
    high = value.astype(BF16)
    rest = value - high.astype(F32)
    middle = rest.astype(BF16)
    return high, middle, (rest - middle.astype(F32)).astype(BF16)


def offsets(count):
    return sorted(range(1, count), key=lambda k: -min(k, count - k))


def near_offsets(count):
    return [k for k in offsets(count) if min(k, count - k) <= count // 4 + 1]


def repeat(count, factor, step):
    def trip(g, _):
        for k in range(factor):
            step(g * factor + k)
        return 0

    lax.fori_loop(0, count // factor, trip, 0)
    for k in range(count // factor * factor, count):
        step(k)


def iota(shape, dim):
    return lax.broadcasted_iota(jnp.int32, shape, dim)


def kernel(
    groups, shards,
    x_hbm, ids_hbm, count_hbm, valid_hbm, temp_hbm, owner_hbm,
    gout, loss_ref, mean_ref,
    ids_ref, count_ref, valid_ref, temp_ref, owner_ref,
    xs, es, dense, turned_x, outbuf, inbuf, head_rows, rest_rows, at_ids, parts,
    stat_send, stat_buf, mean_send, mean_buf,
    in_sem, x_sem, send_sem, route_sem, stat_sem, mean_sem, hello_sem,
):
    cols, pos = x_hbm.shape
    child = ids_ref.shape[0]
    sources = (count_hbm, valid_hbm, temp_hbm, owner_hbm, ids_hbm)
    kept = (count_ref, valid_ref, temp_ref, owner_ref, ids_ref)
    loads = [pltpu.make_async_copy(source, ref, in_sem.at[k]) for k, (source, ref) in enumerate(zip(sources, kept))]
    for load in loads:
        load.start()
    cap = pos // groups
    my_dp = lax.axis_index("dp")
    my_t = lax.axis_index("tensor")
    heads = pl.cdiv(cols, WIDE)

    x_copy = pltpu.make_async_copy(x_hbm, xs.at[pl.ds(0, cols)], x_sem)
    x_copy.start()

    barrier = pltpu.get_barrier_semaphore()

    def peer_of(me, k, count):
        return lax.rem(me + k, count)

    near = near_offsets(shards)
    for k in near:
        pl.semaphore_signal(barrier, inc=1, device_id={"tensor": peer_of(my_t, k, shards)}, device_id_type=MESH)
    for k in offsets(groups):
        pl.semaphore_signal(barrier, inc=1, device_id={"dp": peer_of(my_dp, k, groups)}, device_id_type=MESH)

    for load in loads:
        load.wait()

    powered = jnp.exp(jnp.log(count_ref[...].astype(F32)) * temp_ref[...])
    weights = jnp.where(iota((child, pos), 0) < valid_ref[...], powered, 0.0)
    share = weights / jnp.sum(weights, axis=0, keepdims=True)
    owner = owner_ref[...]
    shift = pos.bit_length() - 1
    owner_dp = lax.shift_right_logical(owner, shift)
    place = lax.bitwise_and(owner, pos - 1)
    member = jnp.where(iota((groups, pos), 0) == owner_dp, 1.0, 0.0).astype(F32)
    before = jnp.where(iota((pos, pos), 0) < iota((pos, pos), 1), 1.0, 0.0).astype(BF16)
    earlier = jnp.dot(member.astype(BF16), before, preferred_element_type=F32)
    rank = jnp.sum(member * earlier, axis=0, keepdims=True)
    target_row = owner_dp * cap + rank.astype(jnp.int32)
    sender = jnp.where(iota((pos, pos), 0) == target_row, 1.0, 0.0).astype(BF16)
    high, middle, low = split(share)
    place_rows = jnp.broadcast_to(place.astype(F32), (child, pos)).astype(BF16)
    none = jnp.zeros_like(low)
    outgoing = dot_nt(sender, jnp.concatenate([high, place_rows], axis=0))
    outgoing = outgoing + dot_nt(sender, jnp.concatenate([middle, none], axis=0))
    outgoing = outgoing + dot_nt(sender, jnp.concatenate([low, none], axis=0))
    outbuf[...] = outgoing.reshape(groups, cap, 2 * child)

    pairs = pos // 2
    local = ids_ref[...] - my_t * cols
    local = jnp.concatenate([local[:, :pairs], local[:, pairs:]], axis=0)
    local = jnp.transpose(local)
    head = lax.shift_right_arithmetic(local, 8)
    head_rows[...] = jnp.where((head >= 0) & (head < heads), head, -1).astype(F32)
    rest_rows[...] = lax.bitwise_and(local, WIDE - 1).astype(F32)

    x_copy.wait()
    xs[cols:, :] = jnp.zeros((xs.shape[0] - cols, pos), xs.dtype)

    def turn(h):
        at = h * WIDE if isinstance(h, int) else pl.multiple_of(h * WIDE, WIDE)
        tile = jnp.transpose(xs[pl.ds(at, WIDE), :]).astype(F32)
        for c in range(WIDE // LANES):
            turned_x[c, pl.ds(h, pos, stride=HEADS), :] = tile[:, c * LANES : (c + 1) * LANES]

    repeat(heads, 3, turn)

    pl.semaphore_wait(barrier, groups - 1 + len(near))

    def cast(source, buffer, slot, sem, axis, me, count):
        for k in offsets(count):
            pltpu.make_async_remote_copy(
                source, buffer.at[me], send_sem.at[slot], sem,
                device_id={axis: peer_of(me, k, count)}, device_id_type=MESH,
            ).start()

    def take(buffer, count, sem):
        piece = buffer.at[pl.ds(0, count)]
        pltpu.make_async_copy(piece, piece, sem).wait()

    for k in offsets(groups):
        peer = peer_of(my_dp, k, groups)
        pltpu.make_async_remote_copy(
            outbuf.at[peer], inbuf.at[my_dp], send_sem.at[0], route_sem,
            device_id={"dp": peer}, device_id_type=MESH,
        ).start()
    for k in near:
        pl.semaphore_signal(hello_sem, inc=1, device_id={"tensor": peer_of(my_t, k, shards)}, device_id_type=MESH)
    inbuf[pl.ds(my_dp, 1)] = outbuf[pl.ds(my_dp, 1)]

    steps = cols // CHUNK

    def part(g):
        return pl.ds(pl.multiple_of(g * CHUNK, CHUNK), CHUNK)

    def fold(value):
        return value.reshape(CHUNK // 8, 8, pos)

    def peaks(values):
        return jnp.max(values.reshape(CHUNK // 16, 16, pos), axis=0)

    def tops(g, top):
        return jnp.maximum(top, peaks(xs[part(g), :]))

    top = lax.fori_loop(1, steps, tops, peaks(xs[0:CHUNK, :]))
    top = jnp.max(top.astype(F32), axis=0, keepdims=True)

    def sums(g, total):
        powers = jnp.exp(xs[part(g), :].astype(F32) - top)
        es[part(g), :] = powers
        return total + jnp.sum(fold(powers), axis=0)

    total = lax.fori_loop(0, steps, sums, jnp.zeros((8, pos), F32))
    own_sum = jnp.sum(total, axis=0, keepdims=True)

    spread_rows = iota((WIDE, LANES), 0).astype(F32).astype(BF16)
    one = jnp.ones((WIDE, LANES), BF16)
    nil = jnp.zeros((WIDE, LANES), BF16)
    head_index = iota((2 * HEADS, LANES), 0)
    lane = iota((2 * HEADS, LANES), 1)
    second = lane >= child
    head_index = jnp.where(
        second, jnp.where(head_index >= HEADS, head_index - HEADS, -2), jnp.where(head_index < HEADS, head_index, -2)
    ).astype(F32)
    batch = 8

    def pair_onehot(rest, k):
        row = rest[k : k + 1].astype(BF16)
        return jnp.where(spread_rows == row, one, nil)

    def pair_rows(at):
        first = pl.multiple_of(at * HEADS, 8)
        return pl.ds(first, HEADS), pl.ds(pl.multiple_of(first + pairs * HEADS, 8), HEADS)

    def joined(ref, rows):
        return jnp.concatenate([ref[c, rows, :] for c in range(WIDE // LANES)], axis=1)

    def gather(g):
        rows = pl.ds(pl.multiple_of(g * batch, batch), batch)
        head, rest = head_rows[rows, :], rest_rows[rows, :]
        found = []
        for k in range(batch):
            upper, lower = pair_rows(g * batch + k)
            values = jnp.concatenate([joined(turned_x, upper), joined(turned_x, lower)], axis=0).astype(BF16)
            reached = jnp.dot(values, pair_onehot(rest, k), preferred_element_type=F32)
            hit = head_index == head[k : k + 1]
            found.append(jnp.sum(jnp.where(hit, reached, 0.0), axis=0, keepdims=True))
        at_ids[rows, :] = jnp.concatenate(found, axis=0)

    repeat(pairs // batch, 8, gather)

    take(inbuf, groups - 1, route_sem)
    turned = jnp.transpose(inbuf[...].reshape(pos, 2 * child))
    label = turned[child : child + 1].astype(jnp.int32)
    receiver = jnp.where(iota((pos, pos), 0) == label, 1.0, 0.0).astype(BF16)
    wanted = [part for part in split(turned[:child]) for _ in range(LANES // child)]
    placed = dot_nt(receiver, jnp.concatenate(wanted, axis=0))
    first_half = iota((pairs, LANES), 1) < child
    target = jnp.zeros((pairs, LANES), F32)
    for k in range(3):
        both = placed[:, k * LANES : (k + 1) * LANES]
        both = jnp.where(first_half, both[:pairs], both[pairs:])
        parts[k] = both
        target = target + both
    product = jnp.transpose(target * at_ids[...])
    own_pick = jnp.concatenate(
        [jnp.sum(product[:child], axis=0, keepdims=True), jnp.sum(product[child:], axis=0, keepdims=True)], axis=1
    )
    own_stats = jnp.concatenate([top, own_sum, own_pick], axis=0)
    stat_send[...] = own_stats
    stat_buf[pl.ds(my_t, 1)] = own_stats.reshape(1, 3, pos)
    pl.semaphore_wait(hello_sem, len(near))
    cast(stat_send, stat_buf, 1, stat_sem, "tensor", my_t, shards)

    def spread(g):
        rows = pl.ds(pl.multiple_of(g * batch, batch), batch)
        head, rest = head_rows[rows, :], rest_rows[rows, :]
        values = [parts[k, rows, :] for k in range(3)]
        for k in range(batch):
            hit = head_index == head[k : k + 1]
            chosen = jnp.concatenate([jnp.where(hit, value[k : k + 1], 0.0) for value in values], axis=0)
            found = dot_nt(chosen.astype(BF16), pair_onehot(rest, k))
            size = 2 * HEADS
            found = found[:size] + found[size : 2 * size] + found[2 * size :]
            upper, lower = pair_rows(g * batch + k)
            for c in range(WIDE // LANES):
                dense[c, upper, :] = found[:HEADS, c * LANES : (c + 1) * LANES]
                dense[c, lower, :] = found[HEADS:, c * LANES : (c + 1) * LANES]

    repeat(pairs // batch, 4, spread)

    take(stat_buf, shards - 1, stat_sem)
    every_top, every_sum = stat_buf[:, 0, :], stat_buf[:, 1, :]
    peak = jnp.max(every_top, axis=0, keepdims=True)
    whole_sum = jnp.sum(every_sum * jnp.exp(every_top - peak), axis=0, keepdims=True)
    loss = peak + jnp.log(whole_sum) - jnp.sum(stat_buf[:, 2, :], axis=0, keepdims=True)
    loss_ref[...] = loss
    own_mean = jnp.broadcast_to(jnp.sum(loss, axis=1, keepdims=True), (1, LANES))
    mean_send[...] = own_mean
    mean_buf[pl.ds(my_dp, 1)] = own_mean.reshape(1, 1, LANES)
    cast(mean_send, mean_buf, 2, mean_sem, "dp", my_dp, groups)

    scale = jnp.exp(top - peak) / whole_sum

    def gradient(h, size=WIDE):
        at = h * WIDE if isinstance(h, int) else pl.multiple_of(h * WIDE, WIDE)
        rows = pl.ds(at, size)
        tile = jnp.transpose(joined(dense, pl.ds(h, pos, stride=HEADS)))[:size]
        gout[rows, :] = (es[rows, :] * scale - tile).astype(gout.dtype)

    whole = cols // WIDE
    repeat(whole, 6, gradient)
    if cols > whole * WIDE:
        gradient(whole, cols - whole * WIDE)

    take(mean_buf, groups - 1, mean_sem)
    mean_ref[...] = jnp.sum(mean_buf[...], axis=0) / (groups * pos)

    take(outbuf, groups - 1, send_sem.at[0])
    take(stat_buf, shards - 1, send_sem.at[1])
    take(mean_buf, groups - 1, send_sem.at[2])


def leave(*refs):
    count = len(refs) // 2
    sems = refs[-1]
    copies = [pltpu.make_async_copy(refs[k], refs[count + k], sems.at[k]) for k in range(count)]
    for copy in copies:
        copy.start()
    for copy in copies:
        copy.wait()


def solution(mesh):
    groups, shards = mesh.shape["dp"], mesh.shape["tensor"]

    def body(logits, child_ids, leaf_counts, leaf_valid, leaf_temp, leaf_owner):
        pos, cols = logits.shape
        child = child_ids.shape[1]
        cap = pos // groups
        padded = pl.cdiv(cols, WIDE) * WIDE
        vmem = pl.BlockSpec(memory_space=pltpu.VMEM)
        anywhere = pl.BlockSpec(memory_space=pl.ANY)
        results = pl.pallas_call(
            functools.partial(kernel, groups, shards),
            out_shape=(
                pltpu.VMEM((cols, pos), logits.dtype),
                pltpu.VMEM((1, pos), F32),
                pltpu.VMEM((1, LANES), F32),
            ),
            in_specs=[anywhere] * 6,
            out_specs=(vmem, vmem, vmem),
            scratch_shapes=[
                pltpu.VMEM((child, pos), jnp.int32),
                pltpu.VMEM((child, pos), jnp.int32),
                pltpu.VMEM((1, pos), jnp.int32),
                pltpu.VMEM((1, pos), F32),
                pltpu.VMEM((1, pos), jnp.int32),
                pltpu.VMEM((padded, pos), logits.dtype),
                pltpu.VMEM((cols, pos), F32),
                pltpu.VMEM((WIDE // LANES, pos * HEADS, LANES), F32),
                pltpu.VMEM((WIDE // LANES, pos * HEADS, LANES), F32),
                pltpu.VMEM((groups, cap, 2 * child), F32),
                pltpu.VMEM((groups, cap, 2 * child), F32),
                pltpu.VMEM((pos // 2, LANES), F32),
                pltpu.VMEM((pos // 2, LANES), F32),
                pltpu.VMEM((pos // 2, LANES), F32),
                pltpu.VMEM((3, pos // 2, LANES), F32),
                pltpu.VMEM((3, pos), F32),
                pltpu.VMEM((shards, 3, pos), F32),
                pltpu.VMEM((1, LANES), F32),
                pltpu.VMEM((groups, 1, LANES), F32),
                pltpu.SemaphoreType.DMA((5,)),
                pltpu.SemaphoreType.DMA,
                pltpu.SemaphoreType.DMA((3,)),
                pltpu.SemaphoreType.DMA,
                pltpu.SemaphoreType.DMA,
                pltpu.SemaphoreType.DMA,
                pltpu.SemaphoreType.REGULAR,
            ],
            compiler_params=pltpu.CompilerParams(collective_id=0, has_side_effects=True),
        )(
            logits.T, child_ids.T, leaf_counts.T,
            leaf_valid.reshape(1, pos), leaf_temp.reshape(1, pos), leaf_owner.reshape(1, pos),
        )
        gradient, row_loss, mean_loss = pl.pallas_call(
            leave,
            out_shape=[jax.ShapeDtypeStruct(value.shape, value.dtype) for value in results],
            in_specs=[vmem] * 3,
            out_specs=[anywhere] * 3,
            scratch_shapes=[pltpu.SemaphoreType.DMA((3,))],
        )(*(pltpu.with_memory_space_constraint(value, pltpu.VMEM) for value in results))
        return gradient.T, row_loss.reshape(pos), mean_loss[0, 0]

    return jax.shard_map(
        body,
        mesh=mesh,
        in_specs=(P("dp", "tensor"), P("dp", None), P("dp", None), P("dp"), P("dp"), P("dp")),
        out_specs=(P("dp", "tensor"), P("dp"), P()),
        check_vma=False,
    )
```
